128 devices in a mesh: gx: 16 (over x, y), gy: 8 (over z, core).
Axes of the slice: x: 4, y: 4, z: 4, core: 2. Of those that a mesh axis runs over, the one named last changes fastest.
Arguments:
- cells: int32 [3, 4194304], P(None, ('gx', 'gy')), may hold values from 0 to 255, as said below
- fractions: float32 [3, 4194304], P(None, ('gx', 'gy')), may hold values from 0 to 1
- charges: float32 [4194304], P(('gx', 'gy')), may hold values from -24 to 24
- influence: float32 [256, 256, 256], P('gx', 'gy'), may hold values from 0.05 to 24, as said below
- shells: int32 [256, 256, 256], P('gx', 'gy'), may hold values from 0 to 255
Outputs:
- potential_hat: float32 [2, 256, 256, 256], P(None, 'gx', 'gy')
- energy: float32 [], replicated
- virial: float32 [3, 3], replicated
- spectrum: float32 [256], replicated
The draws below stay inside these ranges and needn't reach their ends.
Inputs may be any that keep to these rules, and one draw needn't show every extreme that they name: `cells`: atom a belongs to device a // 32768, devices numbered with gy fastest; its y cell lies in that device's block of 16 y planes (block index its gx index) and its z cell in its block of 32 z planes (block index its gy index). `influence`: Positive.
All inputs are finite; a program needn't handle non-finite values.
Results may differ from the reference program's by a relative error of at most 0.0029.
Values sent between devices are 32-bit elements; how exact they have to be, the bound alone decides.
A program may use at most 64 MiB of HBM per device.

```python
import jax
import jax.numpy as jnp
from jax import lax

MESH = 256
SHELLS = 256
SCREEN = 4096
ATOM_DEV = 32768
ATOMS = 4194304
CYD = 16
CZD = 32


def draw_cells(key, part):
    keys = jax.random.split(jax.random.fold_in(key, 11), 3)
    row_index = jnp.arange(ATOMS, dtype=jnp.int32)
    device = row_index // ATOM_DEV
    columns = MESH // CZD
    cell_x = jax.random.randint(keys[0], (ATOMS,), 0, MESH, dtype=jnp.int32)
    cell_y = device // columns * CYD + jax.random.randint(keys[1], (ATOMS,), 0, CYD, dtype=jnp.int32)
    cell_z = device % columns * CZD + jax.random.randint(keys[2], (ATOMS,), 0, CZD, dtype=jnp.int32)
    return jnp.stack([cell_x, cell_y, cell_z]).astype(jnp.int32)


def wave_squared():
    index = jnp.arange(MESH, dtype=jnp.int32)
    wave = jnp.where(index < MESH // 2, index, index - MESH).astype(jnp.float32)
    return wave[:, None, None] ** 2 + wave[None, :, None] ** 2 + wave[None, None, :] ** 2


def draw_influence(key, part):
    squared = wave_squared()
    shape = (MESH, MESH, MESH)
    rough = jnp.exp(jax.random.uniform(jax.random.fold_in(key, 22), shape, jnp.float32, -0.6931, 0.6931))
    return (rough * 8.0 / (1.0 + squared / 2048.0)).astype(jnp.float32)


def draw_shells(key, part):
    metric_tensor = jax.random.randint(jax.random.fold_in(key, 31), (3,), 1, 4, dtype=jnp.int32)
    index = jnp.arange(MESH, dtype=jnp.int32)
    wave = jnp.where(index < MESH // 2, index, index - MESH)
    radius = metric_tensor[0] * wave[:, None, None] ** 2 + metric_tensor[1] * wave[None, :, None] ** 2 + metric_tensor[2] * wave[None, None, :] ** 2
    top_value = (metric_tensor[0] + metric_tensor[1] + metric_tensor[2]) * (MESH // 2) ** 2
    return jnp.minimum(radius * SHELLS // (top_value + 1), SHELLS - 1).astype(jnp.int32)


def block_levels(rng, dims, pieces, smallest, largest):
    def one(dim, parts):
        steps = jax.random.uniform(jax.random.fold_in(jax.random.fold_in(rng, 6), dim), (parts,), jnp.float32, smallest / len(pieces), largest / len(pieces))
        return jnp.repeat(jnp.exp(steps), dims[dim] // parts).reshape((-1,) + (1,) * (len(dims) - dim - 1))

    level = one(*pieces[0])
    for cut in pieces[1:]:
        level = level * one(*cut)
    return level


def centred(rng, shape, width, most, pieces=(), kind=jnp.bfloat16):
    factor_of = block_levels(rng, shape, pieces, -0.22, 0.18) if pieces else 1.0
    values = jax.random.normal(rng, shape, jnp.float32) * width * factor_of
    return jnp.minimum(jnp.maximum(values, -most), most).astype(kind)


def setup_inputs(seed: int = 0) -> dict:
    splits = jax.random.split(jax.random.key(seed), 6)
    return {
        "cells": draw_cells(jax.random.fold_in(splits[5], 71), 0),
        "fractions": jnp.clip(1.0 * jax.random.uniform(splits[1], (3, ATOMS), jnp.float32) ** block_levels(splits[1], (3, ATOMS), ((1, 128),), -0.2, 0.2), 0.0, 1.0),
        "charges": centred(splits[2], (ATOMS,), 4.0, 24.0, ((0, 128),), jnp.float32),
        "influence": draw_influence(jax.random.fold_in(splits[5], 71), 0),
        "shells": draw_shells(jax.random.fold_in(splits[5], 71), 0),
    }


def spline(frac):
    cube = frac * frac * frac
    square = frac * frac
    rest = 1.0 - frac
    return (rest * rest * rest / 6.0, (3.0 * cube - 6.0 * square + 4.0) / 6.0, (-3.0 * cube + 3.0 * square + 3.0 * frac + 1.0) / 6.0, cube / 6.0)


def wave_numbers(index):
    return jnp.where(index < MESH // 2, index, index - MESH).astype(jnp.float32)


def reference(cells, fractions, charges, influence, shells):
    weight_x = spline(fractions[0])
    weight_y = spline(fractions[1])
    weight_z = spline(fractions[2])
    charge_mesh = jnp.zeros((MESH, MESH, MESH), jnp.float32)
    for first in range(4):
        factor_x = lax.optimization_barrier((charges * weight_x[first]).astype(jnp.bfloat16)).astype(jnp.float32)
        index_x = ((cells[0] + first) % MESH).astype(jnp.int32)
        for second in range(4):
            index_y = ((cells[1] + second) % MESH).astype(jnp.int32)
            for third in range(4):
                index_z = ((cells[2] + third) % MESH).astype(jnp.int32)
                factor_yz = lax.optimization_barrier((weight_y[second] * weight_z[third]).astype(jnp.bfloat16)).astype(jnp.float32)
                charge_mesh = charge_mesh.at[index_x, index_y, index_z].add(factor_x * factor_yz)
    transform = jnp.fft.fftn(charge_mesh) / (MESH ** 1.5)
    real_part = jnp.real(transform).astype(jnp.float32)
    imag_part = jnp.imag(transform).astype(jnp.float32)
    index = jnp.arange(MESH, dtype=jnp.int32)
    wave = wave_numbers(index)
    wave_x = wave[:, None, None]
    wave_y = wave[None, :, None]
    wave_z = wave[None, None, :]
    squared = wave_x * wave_x + wave_y * wave_y + wave_z * wave_z
    keep = jnp.where(squared > 0.0, 1.0, 0.0).astype(jnp.float32)
    weight = keep * influence
    potential_hat = jnp.stack([weight * real_part, weight * imag_part])
    power = real_part * real_part + imag_part * imag_part
    influence_weighted = weight * power
    scale = 0.5 / (MESH ** 3)
    whole_sum = jnp.sum(influence_weighted)
    energy = scale * whole_sum
    coef = influence_weighted * 2.0 * (1.0 + squared / SCREEN) / (squared + 1.0 - keep)
    waves = (wave_x, wave_y, wave_z)
    rows_out = []
    for left in range(3):
        entries = []
        for right in range(3):
            cross = jnp.sum(coef * waves[left] * waves[right])
            diagonal = whole_sum if left == right else jnp.float32(0.0)
            entries.append(scale * (diagonal - cross))
        rows_out.append(jnp.stack(entries))
    virial = jnp.stack(rows_out)
    spectrum = jax.ops.segment_sum(power.reshape(-1), shells.reshape(-1).astype(jnp.int32), num_segments=SHELLS) * (SHELLS / (MESH ** 3))
    return potential_hat, energy, virial, spectrum
```

```python
import functools
import math

import jax
import jax.numpy as jnp
from jax import lax
from jax.experimental import pallas as pl
from jax.experimental.pallas import tpu as pltpu
from jax.sharding import Mesh
from jax.sharding import PartitionSpec as P

MESH = 256
SHELLS = 256
SCREEN = 4096
ROWS = 688
CHUNK = 1024
GX = ("gx_0", "gx_1")
GY = ("gy_0", "gy_1")
GX_GY = ("gx_0", "gx_1", "gy_0", "gy_1")


def passed_along(block, axis, distance):
    devices = range(lax.axis_size(axis))
    route = [((i - distance) % len(devices), i) for i in devices]
    return lax.ppermute(block, axis, route)


def cut_along(shard, dim, peers):
    lengths = shard.shape
    parts = shard.reshape(*lengths[:dim], peers, lengths[dim] // peers, *lengths[dim + 1 :])
    return jnp.moveaxis(parts, dim, 0)


def joined_along(parts, dim):
    lengths = list(parts.shape[1:])
    lengths[dim] *= parts.shape[0]
    return jnp.moveaxis(parts, 0, dim).reshape(lengths)


def moved_by_axis(parts, axes, turns):
    inside = parts.shape[1:]
    out = parts.reshape(*(lax.axis_size(a) for a in axes), *inside)
    for k in turns:
        out = lax.all_to_all(out, axes[k], k, k, tiled=True)
    return out.reshape(-1, *inside)


def one_axis_at_a_time(shard, axes, turns, split_dim, concat_dim):
    parts = cut_along(shard, split_dim, lax.axis_size(axes))
    return joined_along(moved_by_axis(parts, axes, turns), concat_dim)


def wave_tables():
    index = jnp.arange(MESH, dtype=jnp.int32)
    phase = index[:, None] * index[None, :] % MESH
    angle = phase.astype(jnp.float32) * (2.0 * math.pi / MESH)
    factor = 1.0 / math.sqrt(MESH)
    return (jnp.cos(angle) * factor, -jnp.sin(angle) * factor)


def spline(frac):
    cube = frac * frac * frac
    square = frac * frac
    rest = 1.0 - frac
    return (
        rest * rest * rest / 6.0,
        (3.0 * cube - 6.0 * square + 4.0) / 6.0,
        (-3.0 * cube + 3.0 * square + 3.0 * frac + 1.0) / 6.0,
        cube / 6.0,
    )


def periodic(cell, weights, rows, dim):
    row = lax.broadcasted_iota(jnp.int32, (rows, 128), 0)
    low = jnp.broadcast_to(cell[dim : dim + 1] & (rows - 1), (rows, 128))
    high = jnp.broadcast_to(cell[dim : dim + 1] // rows, (rows, 128))
    step = (row - low) & (rows - 1)
    table = jnp.zeros((rows, 128), jnp.float32)
    for t in range(4):
        table = jnp.where(step == t, jnp.broadcast_to(weights[t], (rows, 128)), table)
    block = high + jnp.where(row < low, 1, 0)
    return table, block


def build(cells_ref, frac_ref, charge_ref, begin, yz_buf, x_buf, XR=8):
    for tile in range(CHUNK // 128):
        at = pl.ds(pl.multiple_of(begin + tile * 128, 128), 128)
        lanes = pl.ds(tile * 128, 128)
        cell = cells_ref[:, at]
        weights = spline(frac_ref[:, at])
        charge = charge_ref[:, at]
        table, block = periodic(cell, [charge * w[0:1] for w in weights], 8, 0)
        block = block & 31
        for group in range(16):
            pair = [jnp.where(block == 2 * group + h, table, 0.0) for h in range(2)]
            x_buf[pl.ds(16 * group, 16), lanes] = jnp.concatenate(pair, 0).astype(jnp.bfloat16)
        table, block = periodic(cell & 15, [w[1:2] for w in weights], 8, 1)
        wy = [jnp.where(block == h, table, 0.0) for h in range(3)]
        table, block = periodic(cell & 31, [w[2:3] for w in weights], 8, 2)
        wz = [jnp.where(block == h, table, 0.0) for h in range(5)]
        for y in range(19):
            one = jnp.broadcast_to(wy[y // 8][y % 8 : y % 8 + 1], (8, 128))
            for half in range(2):
                pair = jnp.concatenate([one * wz[2 * half], one * wz[2 * half + 1]], 0)
                yz_buf[pl.ds(32 * y + 16 * half, 16), lanes] = pair.astype(jnp.bfloat16)
        tail = []
        for z in range(3):
            one = jnp.broadcast_to(wz[4][z : z + 1], (8, 128))
            tail += [one * wy[h] for h in range(3)]
        tail.append(jnp.zeros((8, 128), jnp.float32))
        for k in range(5):
            pair = jnp.concatenate(tail[2 * k : 2 * k + 2], 0)
            yz_buf[pl.ds(608 + 16 * k, 16), lanes] = pair.astype(jnp.bfloat16)


def product(yz_buf, x_buf):
    return lax.dot_general(
        yz_buf[...], x_buf[...], (((1,), (1,)), ((), ())), preferred_element_type=jnp.float32
    )


def spread_kernel(cells_ref, frac_ref, charge_ref, out_ref, yz0, x0, yz1, x1):
    count = charge_ref.shape[1]
    trips = count // (2 * CHUNK)
    out_ref[...] = jnp.zeros_like(out_ref)
    build(cells_ref, frac_ref, charge_ref, 0, yz0, x0)

    def body(m, carry):
        build(cells_ref, frac_ref, charge_ref, (2 * m + 1) * CHUNK, yz1, x1)
        out_ref[...] += product(yz0, x0)
        nxt = jnp.minimum((2 * m + 2) * CHUNK, count - CHUNK)
        build(cells_ref, frac_ref, charge_ref, nxt, yz0, x0)
        out_ref[...] += product(yz1, x1)
        return carry

    lax.fori_loop(0, trips, body, 0)


def spread(cells, fractions, charges):
    count = charges.shape[0]
    return pl.pallas_call(
        spread_kernel,
        out_shape=jax.ShapeDtypeStruct((ROWS, MESH), jnp.float32),
        in_specs=[pl.BlockSpec(memory_space=pltpu.VMEM)] * 3,
        out_specs=pl.BlockSpec(memory_space=pltpu.VMEM),
        scratch_shapes=[
            pltpu.VMEM((ROWS, CHUNK), jnp.bfloat16),
            pltpu.VMEM((MESH, CHUNK), jnp.bfloat16),
        ] * 2,
        compiler_params=pltpu.CompilerParams(vmem_limit_bytes=48 << 20),
        name="spread",
    )(cells, fractions, charges.reshape(1, count))


def signed(index):
    return jnp.where(index < MESH // 2, index, index - MESH).astype(jnp.float32)

def slab_outputs(real, imag, influence, shells, wave_x, wave_y, wave_z):
    squared = wave_x * wave_x + (wave_y * wave_y + wave_z * wave_z)
    origin = squared > 0.0
    weight = jnp.where(origin, influence, 0.0)
    power = real * real + imag * imag
    value = weight * power
    coef = value * 2.0 * (1.0 + squared * (1.0 / SCREEN)) / jnp.where(origin, squared, 1.0)
    return weight * real, weight * imag, power, value, coef

def onehot_dot(power, shells):
    total = None
    for r in range(4):
        p = power[8 * r : 8 * r + 8]
        s = shells[8 * r : 8 * r + 8]
        high = s >> 4
        low = s & 15
        left = jnp.concatenate([jnp.where(high == b, p, 0.0) for b in range(16)], 0).astype(jnp.bfloat16)
        right = jnp.concatenate([jnp.where(low == b, 1.0, 0.0) for b in range(16)], 0).astype(jnp.bfloat16)
        part = lax.dot_general(left, right, (((1,), (1,)), ((), ())), preferred_element_type=jnp.float32)
        total = part if total is None else total + part
    return total

def epilogue_kernel(s_ref, influence_ref, shells_ref, first_ref, pot_ref, stats_ref, hist, m0, m1, m2, en):
    first_x = first_ref[0]
    first_y = first_ref[1]
    rows = s_ref.shape[2]
    wave_y = signed(first_y + lax.broadcasted_iota(jnp.int32, (rows, MESH), 0))
    wave_z = signed(lax.broadcasted_iota(jnp.int32, (rows, MESH), 1))
    for ref in (hist, m0, m1, m2, en):
        ref[...] = jnp.zeros_like(ref)

    def body(k, carry):
        wave_x = signed(first_x + k)
        pr, pi, power, value, coef = slab_outputs(s_ref[0, k], s_ref[1, k], influence_ref[k], shells_ref[k], wave_x, wave_y, wave_z)
        pot_ref[0, k] = pr
        pot_ref[1, k] = pi
        hist[...] += onehot_dot(power, shells_ref[k])
        en[...] += value
        m0[...] += coef
        m1[...] += coef * wave_x
        m2[...] += coef * (wave_x * wave_x)
        return carry
    lax.fori_loop(0, s_ref.shape[1], body, 0)
    stats_ref[...] = pack_stats(hist[...], en[...], m0[...], m1[...], m2[...], wave_y, wave_z)

def thirds(x):
    a = x.astype(jnp.bfloat16)
    rest = x - a.astype(jnp.float32)
    b = rest.astype(jnp.bfloat16)
    c = (rest - b.astype(jnp.float32)).astype(jnp.bfloat16)
    return a, b, c

def pack_stats(hist, en, m0, m1, m2, wave_y, wave_z):
    row = lax.broadcasted_iota(jnp.int32, (128, 128), 0)
    col = lax.broadcasted_iota(jnp.int32, (128, 128), 1)
    diag = jnp.where((row & 7) == (col & 7), hist, 0.0)
    by_high = jnp.sum(diag.reshape(16, 8, 128), axis=1)
    pick = (lax.broadcasted_iota(jnp.int32, (128, 256), 0) >> 3) == (lax.broadcasted_iota(jnp.int32, (128, 256), 1) & 15)
    pick = jnp.where(pick, 1.0, 0.0).astype(jnp.bfloat16)
    wide = sum(jnp.dot(t, pick, preferred_element_type=jnp.float32) for t in thirds(by_high))
    own = lax.broadcasted_iota(jnp.int32, (16, 256), 0) == (lax.broadcasted_iota(jnp.int32, (16, 256), 1) >> 4)
    spectrum = jnp.sum(jnp.where(own, wide, 0.0), axis=0, keepdims=True)
    terms = [en, m2, m1 * wave_y, m1 * wave_z, m0 * wave_y * wave_y, m0 * wave_y * wave_z, m0 * wave_z * wave_z]
    sub = lax.broadcasted_iota(jnp.int32, (8, 256), 0)
    out = jnp.where(sub == 0, jnp.broadcast_to(spectrum, (8, 256)), 0.0)
    for n, t in enumerate(terms):
        line = jnp.sum(t.reshape(4, 8, 256), axis=0)
        line = jnp.sum(line, axis=0, keepdims=True)
        out = jnp.where(sub == n + 1, jnp.broadcast_to(line, (8, 256)), out)
    return out

def epilogue(structure, influence, shells, first):
    v = pl.BlockSpec(memory_space=pltpu.VMEM)
    rows = influence.shape[1]
    return pl.pallas_call(
        epilogue_kernel,
        out_shape=(jax.ShapeDtypeStruct(structure.shape, jnp.float32), jax.ShapeDtypeStruct((8, 256), jnp.float32)),
        in_specs=[v, v, v, pl.BlockSpec(memory_space=pltpu.SMEM)],
        out_specs=(v, v),
        scratch_shapes=[pltpu.VMEM((128, 128), jnp.float32)] + [pltpu.VMEM((rows, MESH), jnp.float32)] * 4,
        compiler_params=pltpu.CompilerParams(vmem_limit_bytes=48 << 20),
        name="epilogue",
    )(structure, influence, shells, first)


def shards(cells, fractions, charges, influence, shells):
    rows_y = lax.axis_size(GX)
    cols_z = lax.axis_size(GY)
    plane_y = MESH // rows_y
    plane_z = MESH // cols_z
    extended = spread(cells, fractions, charges)
    main = extended[: 19 * 32].reshape(19, 32, MESH)
    tail = extended[19 * 32 : 19 * 32 + 72].reshape(3, 24, MESH)[:, :19].transpose(1, 0, 2)
    spread_mesh = jnp.concatenate([main, tail], 1)
    arrived = passed_along(spread_mesh[plane_y:], GX, 1)
    spread_mesh = spread_mesh[:plane_y].at[:3].add(arrived)
    arrived_z = passed_along(spread_mesh[:, plane_z:], GY, 1)
    spread_mesh = spread_mesh[:, :plane_z].at[:, :3].add(arrived_z)
    keep_y, keep_z = (plane_y, plane_z)
    cosine, minus_sine = wave_tables()
    real_table = jnp.stack([cosine, minus_sine])
    complex_table = jnp.stack([jnp.stack([cosine, -minus_sine]), jnp.stack([minus_sine, cosine])])
    upper_limit = lax.Precision.HIGHEST
    kx_rows = MESH // rows_y
    ky_rows = MESH // cols_z
    flat_mesh = spread_mesh.reshape(keep_y * keep_z, MESH)
    along_x = jnp.einsum("ckx,px->ckp", real_table, flat_mesh, precision=upper_limit)
    moved = lax.all_to_all(along_x[None], GX, split_axis=2, concat_axis=0, tiled=True)
    moved = moved.reshape(rows_y, 2, kx_rows, keep_y, keep_z)
    table_y = complex_table.reshape(2, 2, MESH, rows_y, plane_y)
    along_y = jnp.einsum("ocKst,scktz->okKz", table_y, moved, precision=upper_limit)
    shifted_along_z = one_axis_at_a_time(
        along_y.reshape(2, kx_rows, MESH * keep_z)[None], GY, (1, 0), 3, 0
    )
    shifted_along_z = shifted_along_z.reshape(cols_z, 2, kx_rows, ky_rows, keep_z)
    wave_table_z = complex_table.reshape(2, 2, MESH, cols_z, plane_z)
    structure_factor = jnp.einsum(
        "whzir,ihnqr->wnqz", wave_table_z, shifted_along_z, precision=upper_limit
    )
    first = jnp.stack([lax.axis_index(GX) * kx_rows, lax.axis_index(GY) * ky_rows])
    potential_hat, stats = epilogue(structure_factor, influence, shells, first)
    stats = lax.psum(stats, GX_GY)
    scale = 0.5 / MESH**3
    spectrum = stats[0] * (SHELLS / MESH**3)
    sums = jnp.sum(stats[1:], axis=1)
    cross = jnp.stack([sums[1], sums[2], sums[3], sums[2], sums[4], sums[5], sums[3], sums[5], sums[6]])
    virial = scale * (jnp.eye(3, dtype=jnp.float32) * sums[0] - cross.reshape(3, 3))
    return (potential_hat, scale * sums[0], virial, spectrum)


def solution(mesh):
    finer = Mesh(mesh.devices.reshape(4, 4, 4, 2), ("gx_0", "gx_1", "gy_0", "gy_1"))
    return jax.shard_map(
        shards,
        mesh=finer,
        in_specs=(P(None, GX_GY), P(None, GX_GY), P(GX_GY), P(GX, GY, None), P(GX, GY, None)),
        out_specs=(P(None, GX, GY, None), P(), P(), P()),
        check_vma=False,
    )
```

```python
import functools
import math

import jax
import jax.numpy as jnp
import numpy as np
from jax import lax
from jax.experimental import pallas as pl
from jax.experimental.pallas import tpu as pltpu
from jax.sharding import PartitionSpec as P

MESH = 256
SHELLS = 256
SCREEN = 4096
ROWS = 688
CHUNK = 1024
NX = 16
NY = 8
PARTS = 4
MESHID = pl.DeviceIdType.MESH


def spline(frac):
    cube = frac * frac * frac
    square = frac * frac
    rest = 1.0 - frac
    return (
        rest * rest * rest / 6.0,
        (3.0 * cube - 6.0 * square + 4.0) / 6.0,
        (-3.0 * cube + 3.0 * square + 3.0 * frac + 1.0) / 6.0,
        cube / 6.0,
    )


def periodic(cell, weights, rows, dim):
    row = lax.broadcasted_iota(jnp.int32, (rows, 128), 0)
    low = jnp.broadcast_to(cell[dim : dim + 1] & (rows - 1), (rows, 128))
    high = jnp.broadcast_to(cell[dim : dim + 1] // rows, (rows, 128))
    step = (row - low) & (rows - 1)
    table = jnp.zeros((rows, 128), jnp.float32)
    for t in range(4):
        table = jnp.where(step == t, jnp.broadcast_to(weights[t], (rows, 128)), table)
    block = high + jnp.where(row < low, 1, 0)
    return table, block


def build(cells_ref, frac_ref, charge_ref, begin, yz_buf, x_buf, XR=8):
    for tile in range(CHUNK // 128):
        at = pl.ds(pl.multiple_of(begin + tile * 128, 128), 128)
        lanes = pl.ds(tile * 128, 128)
        cell = cells_ref[:, at]
        weights = spline(frac_ref[:, at])
        charge = charge_ref[:, at]
        table, block = periodic(cell, [charge * w[0:1] for w in weights], 8, 0)
        block = block & 31
        for group in range(16):
            pair = [jnp.where(block == 2 * group + h, table, 0.0) for h in range(2)]
            x_buf[pl.ds(16 * group, 16), lanes] = jnp.concatenate(pair, 0).astype(jnp.bfloat16)
        table, block = periodic(cell & 15, [w[1:2] for w in weights], 8, 1)
        wy = [jnp.where(block == h, table, 0.0) for h in range(3)]
        table, block = periodic(cell & 31, [w[2:3] for w in weights], 8, 2)
        wz = [jnp.where(block == h, table, 0.0) for h in range(5)]
        rows = [jnp.broadcast_to(wy[y // 8][y % 8 : y % 8 + 1], (8, 128)) for y in range(19)]
        order = [(q, y) for q in range(4) for y in range(16)] + [(q, y) for q in range(4) for y in range(16, 19)]
        for k in range(38):
            pair = [rows[y] * wz[q] for q, y in order[2 * k : 2 * k + 2]]
            yz_buf[pl.ds(16 * k, 16), lanes] = jnp.concatenate(pair, 0).astype(jnp.bfloat16)
        tail = []
        for z in range(3):
            one = jnp.broadcast_to(wz[4][z : z + 1], (8, 128))
            tail += [one * wy[h] for h in range(3)]
        tail.append(jnp.zeros((8, 128), jnp.float32))
        for k in range(5):
            pair = jnp.concatenate(tail[2 * k : 2 * k + 2], 0)
            yz_buf[pl.ds(608 + 16 * k, 16), lanes] = pair.astype(jnp.bfloat16)


def product(yz_buf, x_buf):
    return lax.dot_general(
        yz_buf[...], x_buf[...], (((1,), (1,)), ((), ())), preferred_element_type=jnp.float32
    )


def spread_kernel(cells_ref, frac_ref, charge_ref, out_ref, yz0, x0, yz1, x1):
    count = charge_ref.shape[1]
    trips = count // (2 * CHUNK)
    out_ref[...] = jnp.zeros_like(out_ref)
    build(cells_ref, frac_ref, charge_ref, 0, yz0, x0)

    def body(m, carry):
        build(cells_ref, frac_ref, charge_ref, (2 * m + 1) * CHUNK, yz1, x1)
        out_ref[...] += product(yz0, x0)
        nxt = jnp.minimum((2 * m + 2) * CHUNK, count - CHUNK)
        build(cells_ref, frac_ref, charge_ref, nxt, yz0, x0)
        out_ref[...] += product(yz1, x1)
        return carry

    lax.fori_loop(0, trips, body, 0)


def spread(cells, fractions, charges):
    count = charges.shape[0]
    return pl.pallas_call(
        spread_kernel,
        out_shape=jax.ShapeDtypeStruct((ROWS, MESH), jnp.float32),
        in_specs=[pl.BlockSpec(memory_space=pltpu.VMEM)] * 3,
        out_specs=pl.BlockSpec(memory_space=pltpu.VMEM),
        scratch_shapes=[
            pltpu.VMEM((ROWS, CHUNK), jnp.bfloat16),
            pltpu.VMEM((MESH, CHUNK), jnp.bfloat16),
        ] * 2,
        compiler_params=pltpu.CompilerParams(vmem_limit_bytes=48 << 20),
        name="spread",
    )(cells, fractions, charges.reshape(1, count))


def signed(index):
    return jnp.where(index < MESH // 2, index, index - MESH).astype(jnp.float32)

def slab_outputs(real, imag, influence, shells, wave_x, wave_y, wave_z):
    squared = wave_x * wave_x + (wave_y * wave_y + wave_z * wave_z)
    origin = squared > 0.0
    weight = jnp.where(origin, influence, 0.0)
    power = real * real + imag * imag
    value = weight * power
    coef = value * 2.0 * (1.0 + squared * (1.0 / SCREEN)) / jnp.where(origin, squared, 1.0)
    return weight * real, weight * imag, power, value, coef

def onehot_dot(power, shells):
    total = None
    for r in range(4):
        p = power[8 * r : 8 * r + 8]
        s = shells[8 * r : 8 * r + 8]
        high = s >> 4
        low = s & 15
        left = jnp.concatenate([jnp.where(high == b, p, 0.0) for b in range(16)], 0).astype(jnp.bfloat16)
        right = jnp.concatenate([jnp.where(low == b, 1.0, 0.0) for b in range(16)], 0).astype(jnp.bfloat16)
        part = lax.dot_general(left, right, (((1,), (1,)), ((), ())), preferred_element_type=jnp.float32)
        total = part if total is None else total + part
    return total

def thirds(x):
    a = x.astype(jnp.bfloat16)
    rest = x - a.astype(jnp.float32)
    b = rest.astype(jnp.bfloat16)
    c = (rest - b.astype(jnp.float32)).astype(jnp.bfloat16)
    return a, b, c

def pack_stats(hist, en, m0, m1, m2, wave_y, wave_z):
    row = lax.broadcasted_iota(jnp.int32, (128, 128), 0)
    col = lax.broadcasted_iota(jnp.int32, (128, 128), 1)
    diag = jnp.where((row & 7) == (col & 7), hist, 0.0)
    by_high = jnp.sum(diag.reshape(16, 8, 128), axis=1)
    pick = (lax.broadcasted_iota(jnp.int32, (128, 256), 0) >> 3) == (lax.broadcasted_iota(jnp.int32, (128, 256), 1) & 15)
    pick = jnp.where(pick, 1.0, 0.0).astype(jnp.bfloat16)
    wide = sum(jnp.dot(t, pick, preferred_element_type=jnp.float32) for t in thirds(by_high))
    own = lax.broadcasted_iota(jnp.int32, (16, 256), 0) == (lax.broadcasted_iota(jnp.int32, (16, 256), 1) >> 4)
    spectrum = jnp.sum(jnp.where(own, wide, 0.0), axis=0, keepdims=True)
    terms = [en, m2, m1 * wave_y, m1 * wave_z, m0 * wave_y * wave_y, m0 * wave_y * wave_z, m0 * wave_z * wave_z]
    sub = lax.broadcasted_iota(jnp.int32, (8, 256), 0)
    out = jnp.where(sub == 0, jnp.broadcast_to(spectrum, (8, 256)), 0.0)
    for n, t in enumerate(terms):
        line = jnp.sum(t.reshape(4, 8, 256), axis=0)
        line = jnp.sum(line, axis=0, keepdims=True)
        out = jnp.where(sub == n + 1, jnp.broadcast_to(line, (8, 256)), out)
    return out


def split_table(table):
    table = np.asarray(table, np.float64)
    high = table.astype(np.float32).astype(jnp.bfloat16)
    low = (table - high.astype(np.float64)).astype(np.float32).astype(jnp.bfloat16)
    return np.stack([high, low])

def turn(phase, period):
    angle = 2.0 * np.pi * (phase % period) / period
    return np.cos(angle), np.sin(angle)

def complex_block(cosine, sine):
    return np.stack([np.stack([cosine, sine]), np.stack([-sine, cosine])])

def dft_tables():
    small = MESH // NX // PARTS
    k = np.arange(MESH)
    cosine, sine = turn(k[:, None] * k[None, :], MESH)
    along_x = np.stack([cosine, -sine]) / 16.0
    along_x = along_x.reshape(2, NX, PARTS, small, MESH).transpose(2, 1, 0, 3, 4).reshape(512, MESH)
    j = np.arange(16)
    block = complex_block(*turn(j[:, None] * j[None, :], 16))
    first = np.einsum("dcks,ij->dikscj", block, np.eye(small)) / 16.0
    first = first.reshape(2 * small * 16, 16 * 2 * small)
    cosine, sine = turn(j[:, None] * j[None, :], MESH)
    twiddle = np.stack([cosine, -sine])[:, None, :, :, None] * np.ones((1, small, 1, 1, 8))
    twiddle = twiddle.reshape(2, small * 16, 128).astype(np.float32)
    block = complex_block(*turn(j[:, None] * j[None, :], 16)).reshape(2, 2, NY, 2, 16)
    second = np.einsum("dcjky,zw->cyzjdkw", block, np.eye(8)).reshape(256, 256)
    z = np.arange(MESH).reshape(4, 2, 4, 8).transpose(0, 2, 1, 3)
    block = complex_block(*turn(z[..., None] * k, MESH)) / 16.0
    third = block.transpose(2, 3, 1, 4, 5, 0, 6).reshape(512, 512)
    return split_table(along_x), split_table(first), twiddle, split_table(second), split_table(third)

def halves(value):
    high = value.astype(jnp.bfloat16)
    return high, (value - high.astype(jnp.float32)).astype(jnp.bfloat16)

def dot(a, b):
    return jnp.dot(a, b, preferred_element_type=jnp.float32)

def dot_nt(a, b):
    return lax.dot_general(a, b, (((1,), (1,)), ((), ())), preferred_element_type=jnp.float32)

def add_halo(mesh, ext, from_y, from_z, from_corner):
    for q in range(4):
        at = pl.ds(128 * q, 24)
        if q:
            mesh[at] = ext[at] + from_y[pl.ds(24 * q, 24)]
            rest = pl.ds(128 * q + 24, 104)
            mesh[rest] = ext[rest]
    sub = lax.broadcasted_iota(jnp.int32, (8, MESH), 0)
    for y in range(16):
        at = pl.ds(8 * y, 8)
        value = ext[at]
        if y < 3:
            value = value + from_y[at]
        for z in range(3):
            line = from_z[pl.ds(24 * z + y, 1)]
            if y < 3:
                line = line + from_corner[pl.ds(8 * z + y, 1)]
            value = value + jnp.where(sub == z, jnp.broadcast_to(line, (8, MESH)), 0.0)
        mesh[at] = value

def along_x(table, mesh, send):
    high, low = halves(mesh[...])
    for half in range(2):
        at = pl.ds(256 * half, 256)
        out = dot_nt(table[0, at], high) + dot_nt(table[0, at], low) + dot_nt(table[1, at], high)
        send[pl.ds(2 * half, 2)] = out.reshape(2, NX, 8, 512)

def along_y(first, twiddle, second, block, send):
    high, low = halves(block[...].reshape(128, 512))
    out = dot(jnp.concatenate([first[0], first[0]], 1), jnp.concatenate([high, low], 0)) + dot(first[1], high)
    real, imag = out[:64], out[64:]
    tr, ti = twiddle[0], twiddle[1]
    rows = []
    for q in range(4):
        a = real[:, 128 * q : 128 * q + 128]
        b = imag[:, 128 * q : 128 * q + 128]
        rows.append(jnp.concatenate([a * tr - b * ti, a * ti + b * tr], 1))
    high, low = halves(jnp.concatenate(rows, 0))
    out = dot(high, second[0]) + dot(low, second[0]) + dot(high, second[1])
    group = lax.broadcasted_iota(jnp.int32, (64, 128), 1) >> 5
    for j in range(NY):
        total = None
        for q in range(4):
            piece = out[64 * q : 64 * q + 64, 128 * (j // 4) : 128 * (j // 4) + 128]
            shift = (32 * (q - j % 4)) % 128
            if shift:
                piece = pltpu.roll(piece, shift, 1)
            total = piece if total is None else jnp.where(group == q, piece, total)
        send[j] = total

def along_z(third, block):
    odd = ((lax.broadcasted_iota(jnp.int32, (64, 128), 1) >> 3) & 1) == 1
    top, bottom = [], []
    for m in range(4):
        a = block[2 * m]
        b = block[2 * m + 1]
        top.append(jnp.where(odd, pltpu.roll(b, 8, 1), a))
        bottom.append(jnp.where(odd, b, pltpu.roll(a, 120, 1)))
    value = jnp.concatenate([jnp.concatenate(top, 1), jnp.concatenate(bottom, 1)], 0)
    high, low = halves(value)
    return dot(high, third[0]) + dot(low, third[0]) + dot(high, third[1])

def torus(me, d):
    return lax.rem(me // 4 + d // 4, 4) * 4 + lax.rem(lax.rem(me, 4) + d % 4, 4)

def back(me, d):
    return torus(me, (4 - d // 4) % 4 * 4 + (4 - d % 4) % 4)

ORDER = (1, 4, 3, 12, 5, 15, 7, 13, 2, 8, 6, 9, 14, 11, 10)

def mega_kernel(
    ext, influence_hbm, shells_hbm, ax_hbm, first_hbm, twiddle_hbm, second_hbm, third_hbm,
    pot_ref, spectrum_ref, energy_ref, virial_ref,
    influence, shells, ax, first, twiddle, second, third,
    mesh, from_y, from_z, from_corner, send1, recv1, send2, recv2, hist, m0, m1, m2, en, stat, statz, statx,
    load_sem, halo_send, halo_recv, send_sem1, recv_sem1, send_sem2, recv_sem2, send_sem3, recv_sem3,
):
    me_x = lax.axis_index("gx")
    me_y = lax.axis_index("gy")
    right_x, left_x = lax.rem(me_x + 1, NX), lax.rem(me_x + NX - 1, NX)
    right_y, left_y = lax.rem(me_y + 1, NY), lax.rem(me_y + NY - 1, NY)

    loads = [
        pltpu.make_async_copy(a, b, load_sem.at[n])
        for n, (a, b) in enumerate(
            [(ax_hbm, ax), (first_hbm, first), (twiddle_hbm, twiddle), (second_hbm, second), (third_hbm, third),
             (influence_hbm, influence), (shells_hbm, shells)]
        )
    ]
    for load in loads:
        load.start()

    barrier = pltpu.get_barrier_semaphore()
    peers = [{"gx": torus(me_x, d), "gy": me_y} for d in range(1, NX)]
    peers += [{"gx": me_x, "gy": lax.rem(me_y + d, NY)} for d in range(1, NY)]
    peers += [{"gx": right_x, "gy": right_y}, {"gx": left_x, "gy": left_y}]
    for peer in peers:
        pl.semaphore_signal(barrier, inc=1, device_id=peer, device_id_type=MESHID)
    pl.semaphore_wait(barrier, len(peers))

    def remote(src, dst, send_sem, recv_sem, gx, gy):
        return pltpu.make_async_remote_copy(
            src_ref=src, dst_ref=dst, send_sem=send_sem, recv_sem=recv_sem,
            device_id={"gx": gx, "gy": gy}, device_id_type=MESHID,
        )

    halo = [
        remote(ext.at[pl.ds(512, 96)], from_y, halo_send.at[0], halo_recv.at[0], right_x, me_y),
        remote(ext.at[pl.ds(608, 72)], from_z, halo_send.at[1], halo_recv.at[1], me_x, right_y),
    ]
    for z in range(3):
        halo.append(remote(ext.at[pl.ds(608 + 24 * z + 16, 8)], from_corner.at[pl.ds(8 * z, 8)],
                           halo_send.at[2 + z], halo_recv.at[2 + z], right_x, right_y))
    for copy in halo:
        copy.start()
    for copy in halo:
        copy.wait()
    add_halo(mesh, ext, from_y, from_z, from_corner)
    loads[0].wait()
    along_x(ax, mesh, send1)
    exchange1 = []
    for part in range(PARTS):
        group = []
        for d in ORDER:
            to = torus(me_x, d)
            copy = remote(send1.at[part, to], recv1.at[part, me_x], send_sem1.at[part, d], recv_sem1.at[part, d], to, me_y)
            copy.start()
            group.append(copy)
        exchange1.append(group)
    for part in range(PARTS):
        recv1[part, me_x] = send1[part, me_x]
    for load in loads[1:]:
        load.wait()
    exchange2 = []
    for part in range(PARTS):
        for copy in exchange1[part]:
            copy.wait_recv()
        along_y(first, twiddle, second, recv1.at[part], send2.at[part])
        group = []
        for d in range(1, NY):
            to = lax.rem(me_y + d, NY)
            copy = remote(send2.at[part, to], recv2.at[part, me_y], send_sem2.at[part, d], recv_sem2.at[part, d], me_x, to)
            copy.start()
            group.append(copy)
        recv2[part, me_y] = send2[part, me_y]
        exchange2.append(group)

    first_x = me_x * 16
    wave_y = signed(me_y * 32 + lax.broadcasted_iota(jnp.int32, (32, MESH), 0))
    wave_z = signed(lax.broadcasted_iota(jnp.int32, (32, MESH), 1))
    for ref in (hist, m0, m1, m2, en):
        ref[...] = jnp.zeros_like(ref)
    for part in range(PARTS):
        for copy in exchange2[part]:
            copy.wait_recv()
        out = along_z(third, recv2.at[part])
        for n in range(4):
            k = 4 * part + n
            plane = jnp.concatenate([out[16 * n : 16 * n + 16], out[64 + 16 * n : 64 + 16 * n + 16]], 0)
            wave_x = signed(first_x + k)
            pr, pi, power, value, coef = slab_outputs(
                plane[:, :MESH], plane[:, MESH:], influence[k], shells[k], wave_x, wave_y, wave_z)
            pot_ref[0, k] = pr
            pot_ref[1, k] = pi
            hist[...] += onehot_dot(power, shells[k])
            en[...] += value
            m0[...] += coef
            m1[...] += coef * wave_x
            m2[...] += coef * (wave_x * wave_x)
    stat[...] = pack_stats(hist[...], en[...], m0[...], m1[...], m2[...], wave_y, wave_z)

    sums = []
    for d in range(1, NY):
        to = lax.rem(me_y + d, NY)
        sums.append(remote(stat, statz.at[me_y], send_sem3.at[0, d], recv_sem3.at[0, d], me_x, to))
        sums[-1].start()
    statz[me_y] = stat[...]
    for copy in sums:
        copy.wait()
    total = statz[0]
    for n in range(1, NY):
        total = total + statz[n]
    stat[...] = total
    sums = []
    for d in range(1, NX):
        to = torus(me_x, d)
        sums.append(remote(stat, statx.at[me_x], send_sem3.at[1, d], recv_sem3.at[1, d], to, me_y))
        sums[-1].start()
    statx[me_x] = stat[...]
    for copy in sums:
        copy.wait()
    total = statx[0]
    for n in range(1, NX):
        total = total + statx[n]
    spectrum_ref[...] = total[0:1] * (SHELLS / MESH**3)
    scale = 0.5 / MESH**3
    line = jnp.sum(total, axis=1, keepdims=True) * scale
    energy_ref[...] = line[1:2]
    row = lax.broadcasted_iota(jnp.int32, (3, 3), 0)
    col = lax.broadcasted_iota(jnp.int32, (3, 3), 1)
    pair = {(0, 0): 2, (0, 1): 3, (0, 2): 4, (1, 1): 5, (1, 2): 6, (2, 2): 7}
    virial = jnp.where(row == col, jnp.broadcast_to(line[1:2], (3, 3)), 0.0)
    for (a, b), n in pair.items():
        hit = ((row == a) & (col == b)) | ((row == b) & (col == a))
        virial = virial - jnp.where(hit, jnp.broadcast_to(line[n : n + 1], (3, 3)), 0.0)
    virial_ref[...] = virial
    for group in exchange1 + exchange2:
        for copy in group:
            copy.wait_send()


def mega(ext, influence, shells):
    tables = dft_tables()
    f32, bf16 = jnp.float32, jnp.bfloat16
    vmem = pl.BlockSpec(memory_space=pltpu.VMEM)
    anywhere = pl.BlockSpec(memory_space=pl.ANY)
    return pl.pallas_call(
        mega_kernel,
        out_shape=(
            jax.ShapeDtypeStruct((2,) + influence.shape, f32),
            jax.ShapeDtypeStruct((1, SHELLS), f32),
            jax.ShapeDtypeStruct((1, 1), f32),
            jax.ShapeDtypeStruct((3, 3), f32),
        ),
        in_specs=[vmem] + [anywhere] * 7,
        out_specs=(vmem,) * 4,
        scratch_shapes=[
            pltpu.VMEM(influence.shape, f32), pltpu.VMEM(shells.shape, jnp.int32),
            pltpu.VMEM((2, 512, MESH), bf16), pltpu.VMEM((2, 128, 128), bf16), pltpu.VMEM((2, 64, 128), f32),
            pltpu.VMEM((2, 256, 256), bf16), pltpu.VMEM((2, 512, 512), bf16),
            pltpu.VMEM((512, MESH), f32), pltpu.VMEM((96, MESH), f32), pltpu.VMEM((72, MESH), f32), pltpu.VMEM((24, MESH), f32),
            pltpu.VMEM((PARTS, NX, 8, 512), f32), pltpu.VMEM((PARTS, NX, 8, 512), f32),
            pltpu.VMEM((PARTS, NY, 64, 128), f32), pltpu.VMEM((PARTS, NY, 64, 128), f32),
            pltpu.VMEM((128, 128), f32)] + [pltpu.VMEM((32, MESH), f32)] * 4 + [
            pltpu.VMEM((8, MESH), f32), pltpu.VMEM((NY, 8, MESH), f32), pltpu.VMEM((NX, 8, MESH), f32),
            pltpu.SemaphoreType.DMA((7,)), pltpu.SemaphoreType.DMA((5,)), pltpu.SemaphoreType.DMA((5,)),
            pltpu.SemaphoreType.DMA((PARTS, NX)), pltpu.SemaphoreType.DMA((PARTS, NX)),
            pltpu.SemaphoreType.DMA((PARTS, NY)), pltpu.SemaphoreType.DMA((PARTS, NY)),
            pltpu.SemaphoreType.DMA((2, NX)), pltpu.SemaphoreType.DMA((2, NX)),
        ],
        compiler_params=pltpu.CompilerParams(collective_id=0, has_side_effects=True, vmem_limit_bytes=56 << 20),
        name="transform",
    )(ext, influence, shells, *tables)


def shards(cells, fractions, charges, influence, shells):
    extended = spread(cells, fractions, charges)
    potential_hat, spectrum, energy, virial = mega(extended, influence, shells)
    return potential_hat, energy.reshape(()), virial, spectrum.reshape(SHELLS)


def solution(mesh):
    both = ("gx", "gy")
    return jax.shard_map(
        shards,
        mesh=mesh,
        in_specs=(P(None, both), P(None, both), P(both), P("gx", "gy", None), P("gx", "gy", None)),
        out_specs=(P(None, "gx", "gy", None), P(), P(), P()),
        check_vma=False,
    )
```

```python
import functools
import math

import jax
import jax.numpy as jnp
import numpy as np
from jax import lax
from jax.experimental import pallas as pl
from jax.experimental.pallas import tpu as pltpu
from jax.sharding import PartitionSpec as P

MESH = 256
SHELLS = 256
SCREEN = 4096
ROWS = 688
CHUNK = 2048
NX = 16
NY = 8
PARTS = 4
SMALL = 16 // PARTS
VLIM = 44
MESHID = pl.DeviceIdType.MESH


def spline(frac):
    cube = frac * frac * frac
    square = frac * frac
    rest = 1.0 - frac
    return (
        rest * rest * rest * (1.0 / 6.0),
        (3.0 * cube - 6.0 * square + 4.0) * (1.0 / 6.0),
        (-3.0 * cube + 3.0 * square + 3.0 * frac + 1.0) * (1.0 / 6.0),
        cube * (1.0 / 6.0),
    )


def wide(line):
    return jnp.broadcast_to(line, (8, 128))


def periodic(low, high, weights, dim):
    row = lax.broadcasted_iota(jnp.int32, (8, 128), 0)
    ahead = row - wide(low[dim : dim + 1])
    step = ahead & 7
    table = jnp.where(step == 3, wide(weights[3]), 0.0)
    for t in range(3):
        table = jnp.where(step == t, wide(weights[t]), table)
    block = wide(high[dim : dim + 1]) + lax.shift_right_logical(ahead, 31)
    return table, block


def build(cells_ref, frac_ref, charge_ref, begin, yz_buf, x_buf):
    dims = lax.broadcasted_iota(jnp.int32, (3, 128), 0)
    inside = jnp.where(dims == 0, 255, jnp.where(dims == 1, 15, 31))
    for tile in range(CHUNK // 128):
        at = pl.ds(pl.multiple_of(begin + tile * 128, 128), 128)
        cell = cells_ref[:, at] & inside
        low = cell & 7
        high = lax.shift_right_logical(cell, 3)
        weights = spline(frac_ref[:, at])
        charge = charge_ref[:, at]
        table, block = periodic(low, high, [charge * w[0:1] for w in weights], 0)
        block = block & 31
        for group in range(32):
            x_buf[tile, pl.ds(8 * group, 8)] = jnp.where(block == group, table, 0.0)
        table, block = periodic(low, high, [w[1:2] for w in weights], 1)
        wy = [jnp.where(block == h, table, 0.0) for h in range(3)]
        table, block = periodic(low, high, [w[2:3] for w in weights], 2)
        wz = [jnp.where(block == h, table, 0.0) for h in range(5)]
        for y in range(19):
            one = wide(wy[y // 8][y % 8 : y % 8 + 1])
            for q in range(4):
                group = 16 * q + y if y < 16 else 64 + 3 * q + y - 16
                yz_buf[tile, pl.ds(8 * group, 8)] = one * wz[q]
        for z in range(3):
            one = wide(wz[4][z : z + 1])
            for h in range(3):
                yz_buf[tile, pl.ds(608 + 24 * z + 8 * h, 8)] = one * wy[h]


def product(yz_buf, x_buf):
    total = None
    for k in range(CHUNK // 256):
        rows = jnp.concatenate([yz_buf[2 * k], yz_buf[2 * k + 1]], 1)
        columns = jnp.concatenate([x_buf[2 * k], x_buf[2 * k + 1]], 1)
        part = lax.dot_general(rows, columns, (((1,), (1,)), ((), ())), preferred_element_type=jnp.float32)
        total = part if total is None else total + part
    return total


def atom_loads(cells_hbm, frac_hbm, charge_hbm, cells_ref, frac_ref, charge_ref, sems):
    count = charge_ref.shape[1]
    pieces = [pl.ds(0, CHUNK), pl.ds(CHUNK, count - CHUNK)]
    pairs = [(cells_hbm, cells_ref), (frac_hbm, frac_ref), (charge_hbm, charge_ref)]
    return [
        [pltpu.make_async_copy(a.at[:, piece], b.at[:, piece], sems.at[n, m]) for m, (a, b) in enumerate(pairs)]
        for n, piece in enumerate(pieces)
    ]


def spread_atoms(pieces, cells_ref, frac_ref, charge_ref, out_ref, yz0, x0, yz1, x1):
    count = charge_ref.shape[1]
    trips = count // (2 * CHUNK)

    out_ref[...] = jnp.zeros_like(out_ref)
    for yz in (yz0, yz1):
        yz[:, pl.ds(ROWS - 8, 8), :] = jnp.zeros((CHUNK // 128, 8, 128), jnp.float32)
    for load in pieces[0]:
        load.wait()
    build(cells_ref, frac_ref, charge_ref, 0, yz0, x0)
    for load in pieces[1]:
        load.wait()

    def body(m, carry):
        build(cells_ref, frac_ref, charge_ref, (2 * m + 1) * CHUNK, yz1, x1)
        out_ref[...] += product(yz0, x0)
        nxt = jnp.minimum((2 * m + 2) * CHUNK, count - CHUNK)
        build(cells_ref, frac_ref, charge_ref, nxt, yz0, x0)
        out_ref[...] += product(yz1, x1)
        return carry

    lax.fori_loop(0, trips - 1, body, 0)
    build(cells_ref, frac_ref, charge_ref, count - CHUNK, yz1, x1)
    out_ref[...] += product(yz0, x0)
    out_ref[...] += product(yz1, x1)


def signed(index):
    return jnp.where(index < MESH // 2, index, index - MESH).astype(jnp.float32)

def slab_outputs(real, imag, influence, shells, wave_x, wave_y, wave_z):
    squared = wave_x * wave_x + (wave_y * wave_y + wave_z * wave_z)
    origin = squared > 0.0
    weight = jnp.where(origin, influence, 0.0)
    power = real * real + imag * imag
    value = weight * power
    coef = value * 2.0 * (1.0 + squared * (1.0 / SCREEN)) / jnp.where(origin, squared, 1.0)
    return weight * real, weight * imag, power, value, coef

def onehot_dot(power, shells):
    total = None
    for r in range(4):
        p = power[8 * r : 8 * r + 8]
        s = shells[8 * r : 8 * r + 8]
        high = s >> 4
        low = s & 15
        left = jnp.concatenate([jnp.where(high == b, p, 0.0) for b in range(16)], 0).astype(jnp.bfloat16)
        right = jnp.concatenate([jnp.where(low == b, 1.0, 0.0) for b in range(16)], 0).astype(jnp.bfloat16)
        part = lax.dot_general(left, right, (((1,), (1,)), ((), ())), preferred_element_type=jnp.float32)
        total = part if total is None else total + part
    return total

def thirds(x):
    a = x.astype(jnp.bfloat16)
    rest = x - a.astype(jnp.float32)
    b = rest.astype(jnp.bfloat16)
    c = (rest - b.astype(jnp.float32)).astype(jnp.bfloat16)
    return a, b, c

def pack_stats(hist, en, m0, m1, m2, wave_y, wave_z):
    row = lax.broadcasted_iota(jnp.int32, (128, 128), 0)
    col = lax.broadcasted_iota(jnp.int32, (128, 128), 1)
    diag = jnp.where((row & 7) == (col & 7), hist, 0.0)
    by_high = jnp.sum(diag.reshape(16, 8, 128), axis=1)
    pick = (lax.broadcasted_iota(jnp.int32, (128, 256), 0) >> 3) == (lax.broadcasted_iota(jnp.int32, (128, 256), 1) & 15)
    pick = jnp.where(pick, 1.0, 0.0).astype(jnp.bfloat16)
    wide = sum(jnp.dot(t, pick, preferred_element_type=jnp.float32) for t in thirds(by_high))
    own = lax.broadcasted_iota(jnp.int32, (16, 256), 0) == (lax.broadcasted_iota(jnp.int32, (16, 256), 1) >> 4)
    spectrum = jnp.sum(jnp.where(own, wide, 0.0), axis=0, keepdims=True)
    terms = [en, m2, m1 * wave_y, m1 * wave_z, m0 * wave_y * wave_y, m0 * wave_y * wave_z, m0 * wave_z * wave_z]
    sub = lax.broadcasted_iota(jnp.int32, (8, 128), 0)
    lane = lax.broadcasted_iota(jnp.int32, (8, 128), 1)
    out = jnp.where(sub == 0, jnp.broadcast_to(spectrum[:, :128], (8, 128)), 0.0)
    out = jnp.where(sub == 1, jnp.broadcast_to(spectrum[:, 128:], (8, 128)), out)
    for n, t in enumerate(terms):
        line = jnp.sum(t.reshape(4, 8, MESH), axis=0)
        line = line[:, :128] + line[:, 128:]
        line = jnp.sum(jnp.sum(line, axis=0, keepdims=True), axis=1, keepdims=True)
        out = jnp.where((sub == 2) & (lane == n), jnp.broadcast_to(line, (8, 128)), out)
    return out


def split_table(table):
    table = np.asarray(table, np.float64)
    high = table.astype(np.float32).astype(jnp.bfloat16)
    low = (table - high.astype(np.float64)).astype(np.float32).astype(jnp.bfloat16)
    return np.stack([high, low])

def turn(phase, period):
    angle = 2.0 * np.pi * (phase % period) / period
    return np.cos(angle), np.sin(angle)

def complex_block(cosine, sine):
    return np.stack([np.stack([cosine, sine]), np.stack([-sine, cosine])])

def dft_tables():
    small = MESH // NX // PARTS
    k = np.arange(MESH)
    cosine, sine = turn(k[:, None] * k[None, :], MESH)
    along_x = np.stack([cosine, -sine]) / 16.0
    along_x = along_x.reshape(2, NX, PARTS, small, MESH).transpose(2, 1, 0, 3, 4).reshape(512, MESH)
    j = np.arange(16)
    block = complex_block(*turn(j[:, None] * j[None, :], 16))
    first = np.einsum("dcks,ij->dikscj", block, np.eye(small)) / 16.0
    first = first.reshape(2 * small * 16, 16 * 2 * small)
    cosine, sine = turn(j[:, None] * j[None, :], MESH)
    twiddle = np.stack([cosine, -sine])[:, None, :, :, None] * np.ones((1, small, 1, 1, 8))
    twiddle = twiddle.reshape(2, small * 16, 128).astype(np.float32)
    block = complex_block(*turn(j[:, None] * j[None, :], 16)).reshape(2, 2, NY, 2, 16)
    second = np.einsum("dcjky,zw->cyzjdkw", block, np.eye(8)).reshape(256, 256)
    z = np.arange(MESH).reshape(4, 2, 4, 8).transpose(0, 2, 1, 3)
    block = complex_block(*turn(z[..., None] * k, MESH)) / 16.0
    third = block.transpose(2, 3, 1, 4, 5, 0, 6).reshape(512, 512)
    return split_table(along_x), split_table(first), twiddle, split_table(second), split_table(third)

def halves(value):
    high = value.astype(jnp.bfloat16)
    return high, (value - high.astype(jnp.float32)).astype(jnp.bfloat16)

def dot(a, b):
    return jnp.dot(a, b, preferred_element_type=jnp.float32)

def dot_nt(a, b):
    return lax.dot_general(a, b, (((1,), (1,)), ((), ())), preferred_element_type=jnp.float32)

def add_halo(mesh, ext, from_y, from_z, from_corner):
    for q in range(4):
        at = pl.ds(128 * q, 24)
        if q:
            mesh[at] = ext[at] + from_y[pl.ds(24 * q, 24)]
            rest = pl.ds(128 * q + 24, 104)
            mesh[rest] = ext[rest]
    sub = lax.broadcasted_iota(jnp.int32, (8, MESH), 0)
    for y in range(16):
        at = pl.ds(8 * y, 8)
        value = ext[at]
        if y < 3:
            value = value + from_y[at]
        for z in range(3):
            line = from_z[pl.ds(24 * z + y, 1)]
            if y < 3:
                line = line + from_corner[pl.ds(8 * z + y, 1)]
            value = value + jnp.where(sub == z, jnp.broadcast_to(line, (8, MESH)), 0.0)
        mesh[at] = value

def along_x(table, mesh, send, ready):
    high, low = halves(mesh[...])
    for half in range(2):
        at = pl.ds(256 * half, 256)
        out = dot_nt(table[0, at], high) + dot_nt(table[0, at], low) + dot_nt(table[1, at], high)
        some = pl.ds(PARTS // 2 * half, PARTS // 2)
        send[some] = out.reshape(PARTS // 2, NX, 2 * SMALL, 512)
        ready(half)

def along_y(first, twiddle, second, block, send):
    high, low = halves(block[...].reshape(32 * SMALL, 512))
    out = dot(jnp.concatenate([first[0], first[0]], 1), jnp.concatenate([high, low], 0)) + dot(first[1], high)
    rows = 16 * SMALL
    real, imag = out[:rows], out[rows:]
    tr, ti = twiddle[0], twiddle[1]
    lines = []
    for q in range(4):
        a = real[:, 128 * q : 128 * q + 128]
        b = imag[:, 128 * q : 128 * q + 128]
        lines.append(jnp.concatenate([a * tr - b * ti, a * ti + b * tr], 1))
    high, low = halves(jnp.concatenate(lines, 0))
    out = dot(high, second[0]) + dot(low, second[0]) + dot(high, second[1])
    group = lax.broadcasted_iota(jnp.int32, (rows, 128), 1) >> 5
    for j in range(NY):
        total = None
        for q in range(4):
            piece = out[rows * q : rows * q + rows, 128 * (j // 4) : 128 * (j // 4) + 128]
            shift = (32 * (q - j % 4)) % 128
            if shift:
                piece = pltpu.roll(piece, shift, 1)
            total = piece if total is None else jnp.where(group == q, piece, total)
        send[j] = total

def along_z(third, block):
    odd = ((lax.broadcasted_iota(jnp.int32, (16 * SMALL, 128), 1) >> 3) & 1) == 1
    top, bottom = [], []
    for m in range(4):
        a = block[2 * m]
        b = block[2 * m + 1]
        top.append(jnp.where(odd, pltpu.roll(b, 8, 1), a))
        bottom.append(jnp.where(odd, b, pltpu.roll(a, 120, 1)))
    value = jnp.concatenate([jnp.concatenate(top, 1), jnp.concatenate(bottom, 1)], 0)
    high, low = halves(value)
    return dot(high, third[0]) + dot(low, third[0]) + dot(high, third[1])

def torus(me, d):
    return lax.rem(me // 4 + d // 4, 4) * 4 + lax.rem(lax.rem(me, 4) + d % 4, 4)

def back(me, d):
    return torus(me, (4 - d // 4) % 4 * 4 + (4 - d % 4) % 4)

ORDER = (10, 11, 14, 9, 6, 2, 8, 5, 15, 7, 13, 1, 4, 3, 12)
ORDER_Y = (4, 3, 5, 2, 6, 7, 1)
ORDER_SUM = (10, 11, 14, 9, 6, 2, 8, 5, 15, 7, 13, 1, 4, 3, 12)


def whole_kernel(
    cells_hbm, frac_hbm, charge_hbm, influence_hbm, shells_hbm, ax_hbm, first_hbm, twiddle_hbm, second_hbm, third_hbm,
    pot_ref, result_ref,
    cells_ref, frac_ref, charge_ref, yz0, x0, yz1, x1, ext,
    influence, shells, ax, first, twiddle, second, third,
    mesh, from_y, from_z, from_corner, send1, recv1, send2, recv2, hist, m0, m1, m2, en, stat, statz, statx,
    atom_sem, load_sem, halo_send, halo_recv, send_sem1, recv_sem1, send_sem2, recv_sem2, send_sem3, recv_sem3,
):
    me_x = lax.axis_index("gx")
    me_y = lax.axis_index("gy")
    right_x, left_x = lax.rem(me_x + 1, NX), lax.rem(me_x + NX - 1, NX)
    right_y, left_y = lax.rem(me_y + 1, NY), lax.rem(me_y + NY - 1, NY)

    pieces = atom_loads(cells_hbm, frac_hbm, charge_hbm, cells_ref, frac_ref, charge_ref, atom_sem)
    for piece in pieces:
        for load in piece:
            load.start()
    loads = [
        pltpu.make_async_copy(a, b, load_sem.at[n])
        for n, (a, b) in enumerate(
            [(ax_hbm, ax), (first_hbm, first), (twiddle_hbm, twiddle), (second_hbm, second), (third_hbm, third),
             (influence_hbm, influence), (shells_hbm, shells)]
        )
    ]
    for load in loads:
        load.start()

    barrier = pltpu.get_barrier_semaphore()
    peers = [{"gx": torus(me_x, d), "gy": me_y} for d in range(1, NX)]
    peers += [{"gx": me_x, "gy": lax.rem(me_y + d, NY)} for d in range(1, NY)]
    peers += [{"gx": right_x, "gy": right_y}, {"gx": left_x, "gy": left_y}]
    for peer in peers:
        pl.semaphore_signal(barrier, inc=1, device_id=peer, device_id_type=MESHID)
    spread_atoms(pieces, cells_ref, frac_ref, charge_ref, ext, yz0, x0, yz1, x1)
    pl.semaphore_wait(barrier, len(peers))

    def remote(src, dst, send_sem, recv_sem, gx, gy):
        return pltpu.make_async_remote_copy(
            src_ref=src, dst_ref=dst, send_sem=send_sem, recv_sem=recv_sem,
            device_id={"gx": gx, "gy": gy}, device_id_type=MESHID,
        )

    halo = [
        remote(ext.at[pl.ds(512, 96)], from_y, halo_send.at[0], halo_recv.at[0], right_x, me_y),
        remote(ext.at[pl.ds(608, 72)], from_z, halo_send.at[1], halo_recv.at[1], me_x, right_y),
    ]
    for z in range(3):
        halo.append(remote(ext.at[pl.ds(608 + 24 * z + 16, 8)], from_corner.at[pl.ds(8 * z, 8)],
                           halo_send.at[2 + z], halo_recv.at[2 + z], right_x, right_y))
    for copy in halo:
        copy.start()
    for copy in halo:
        copy.wait()
    add_halo(mesh, ext, from_y, from_z, from_corner)
    loads[0].wait()
    exchange1 = []

    def ready(half):
        for part in range(PARTS // 2 * half, PARTS // 2 * (half + 1)):
            group = []
            for d in ORDER:
                to = torus(me_x, d)
                group.append(remote(
                    send1.at[part, to], recv1.at[part, me_x], send_sem1.at[part, d], recv_sem1.at[part, d], to, me_y))
                group[-1].start()
            exchange1.append(group)

    along_x(ax, mesh, send1, ready)
    for part in range(PARTS):
        recv1[part, me_x] = send1[part, me_x]
    for load in loads[1:]:
        load.wait()
    exchange2 = []
    for part in range(PARTS):
        for copy in exchange1[part]:
            copy.wait_recv()
        along_y(first, twiddle, second, recv1.at[part], send2.at[part])
        group = []
        for d in ORDER_Y:
            to = lax.rem(me_y + d, NY)
            copy = remote(send2.at[part, to], recv2.at[part, me_y], send_sem2.at[part, d], recv_sem2.at[part, d], me_x, to)
            copy.start()
            group.append(copy)
        recv2[part, me_y] = send2[part, me_y]
        exchange2.append(group)

    first_x = me_x * 16
    wave_y = signed(me_y * 32 + lax.broadcasted_iota(jnp.int32, (32, MESH), 0))
    wave_z = signed(lax.broadcasted_iota(jnp.int32, (32, MESH), 1))
    for ref in (hist, m0, m1, m2, en):
        ref[...] = jnp.zeros_like(ref)
    for part in range(PARTS):
        for copy in exchange2[part]:
            copy.wait_recv()
        out = along_z(third, recv2.at[part])
        for n in range(SMALL):
            k = SMALL * part + n
            low = 16 * (SMALL + n)
            plane = jnp.concatenate([out[16 * n : 16 * n + 16], out[low : low + 16]], 0)
            wave_x = signed(first_x + k)
            pr, pi, power, value, coef = slab_outputs(
                plane[:, :MESH], plane[:, MESH:], influence[k], shells[k], wave_x, wave_y, wave_z)
            pot_ref[0, k] = pr
            pot_ref[1, k] = pi
            hist[...] += onehot_dot(power, shells[k])
            en[...] += value
            m0[...] += coef
            m1[...] += coef * wave_x
            m2[...] += coef * (wave_x * wave_x)
    stat[...] = pack_stats(hist[...], en[...], m0[...], m1[...], m2[...], wave_y, wave_z)

    sums = []
    for d in ORDER_Y:
        to = lax.rem(me_y + d, NY)
        sums.append(remote(stat, statz.at[me_y], send_sem3.at[0, d], recv_sem3.at[0, d], me_x, to))
        sums[-1].start()
    statz[me_y] = stat[...]
    for copy in sums:
        copy.wait()
    total = statz[0]
    for n in range(1, NY):
        total = total + statz[n]
    stat[...] = total
    sums = []
    for d in ORDER_SUM:
        to = torus(me_x, d)
        sums.append(remote(stat, statx.at[me_x], send_sem3.at[1, d], recv_sem3.at[1, d], to, me_y))
        sums[-1].start()
    statx[me_x] = stat[...]
    for copy in sums:
        copy.wait()
    total = statx[0]
    for n in range(1, NX):
        total = total + statx[n]
    result_ref[...] = total
    for group in exchange1 + exchange2:
        for copy in group:
            copy.wait_send()


def last_kernel(pot, result, pot_hbm, spectrum_ref, energy_ref, virial_ref, sem):
    slabs = [(c, pl.ds(4 * n, 4)) for c in range(2) for n in range(4)]
    writes = [pltpu.make_async_copy(pot.at[at], pot_hbm.at[at], sem.at[n]) for n, at in enumerate(slabs)]
    for write in writes:
        write.start()
    total = result[...]
    spectrum_ref[:, pl.ds(0, 128)] = total[0:1] * (SHELLS / MESH**3)
    spectrum_ref[:, pl.ds(128, 128)] = total[1:2] * (SHELLS / MESH**3)
    line = total[2:3] * (0.5 / MESH**3)
    energy_ref[...] = line[:, 0:1]
    row = lax.broadcasted_iota(jnp.int32, (3, 3), 0)
    col = lax.broadcasted_iota(jnp.int32, (3, 3), 1)
    pair = {(0, 0): 1, (0, 1): 2, (0, 2): 3, (1, 1): 4, (1, 2): 5, (2, 2): 6}
    virial = jnp.where(row == col, jnp.broadcast_to(line[:, 0:1], (3, 3)), 0.0)
    for (a, b), n in pair.items():
        hit = ((row == a) & (col == b)) | ((row == b) & (col == a))
        virial = virial - jnp.where(hit, jnp.broadcast_to(line[:, n : n + 1], (3, 3)), 0.0)
    virial_ref[...] = virial
    for write in writes:
        write.wait()


def shards(cells, fractions, charges, influence, shells):
    tables = dft_tables()
    count = charges.shape[0]
    f32, bf16 = jnp.float32, jnp.bfloat16
    vmem = pl.BlockSpec(memory_space=pltpu.VMEM)
    anywhere = pl.BlockSpec(memory_space=pl.ANY)
    dma = pltpu.SemaphoreType.DMA
    pot, result = pl.pallas_call(
        whole_kernel,
        out_shape=(jax.ShapeDtypeStruct((2,) + influence.shape, f32), jax.ShapeDtypeStruct((8, 128), f32)),
        in_specs=[anywhere] * 10,
        out_specs=(vmem, vmem),
        scratch_shapes=[
            pltpu.VMEM((3, count), jnp.int32), pltpu.VMEM((3, count), f32), pltpu.VMEM((1, count), f32),
        ] + [pltpu.VMEM((CHUNK // 128, ROWS, 128), f32), pltpu.VMEM((CHUNK // 128, MESH, 128), f32)] * 2 + [
            pltpu.VMEM((ROWS, MESH), f32),
            pltpu.VMEM(influence.shape, f32), pltpu.VMEM(shells.shape, jnp.int32),
            pltpu.VMEM((2, 512, MESH), bf16), pltpu.VMEM((2, 32 * SMALL, 32 * SMALL), bf16), pltpu.VMEM((2, 16 * SMALL, 128), f32),
            pltpu.VMEM((2, 256, 256), bf16), pltpu.VMEM((2, 512, 512), bf16),
            pltpu.VMEM((512, MESH), f32), pltpu.VMEM((96, MESH), f32), pltpu.VMEM((72, MESH), f32), pltpu.VMEM((24, MESH), f32),
            pltpu.VMEM((PARTS, NX, 2 * SMALL, 512), f32), pltpu.VMEM((PARTS, NX, 2 * SMALL, 512), f32),
            pltpu.VMEM((PARTS, NY, 16 * SMALL, 128), f32), pltpu.VMEM((PARTS, NY, 16 * SMALL, 128), f32),
            pltpu.VMEM((128, 128), f32)] + [pltpu.VMEM((32, MESH), f32)] * 4 + [
            pltpu.VMEM((8, 128), f32), pltpu.VMEM((NY, 8, 128), f32), pltpu.VMEM((NX, 8, 128), f32),
            dma((2, 3)), dma((7,)), dma((5,)), dma((5,)),
            dma((PARTS, NX)), dma((PARTS, NX)), dma((PARTS, NY)), dma((PARTS, NY)), dma((2, NX)), dma((2, NX)),
        ],
        compiler_params=pltpu.CompilerParams(collective_id=0, has_side_effects=True, vmem_limit_bytes=VLIM << 20),
        name="whole",
    )(*[pltpu.with_memory_space_constraint(a, pltpu.HBM) for a in (cells, fractions, charges.reshape(1, count), influence, shells, *tables)])
    potential_hat, spectrum, energy, virial = pl.pallas_call(
        last_kernel,
        out_shape=(
            jax.ShapeDtypeStruct(pot.shape, f32),
            jax.ShapeDtypeStruct((1, SHELLS), f32),
            jax.ShapeDtypeStruct((1, 1), f32),
            jax.ShapeDtypeStruct((3, 3), f32),
        ),
        in_specs=[vmem] * 2,
        out_specs=(anywhere, vmem, vmem, vmem),
        scratch_shapes=[dma((8,))],
        compiler_params=pltpu.CompilerParams(vmem_limit_bytes=8 << 20),
        name="last",
    )(pot, result)
    return potential_hat, energy.reshape(()), virial, spectrum.reshape(SHELLS)


def solution(mesh):
    both = ("gx", "gy")
    return jax.shard_map(
        shards,
        mesh=mesh,
        in_specs=(P(None, both), P(None, both), P(both), P("gx", "gy", None), P("gx", "gy", None)),
        out_specs=(P(None, "gx", "gy", None), P(), P(), P()),
        check_vma=False,
    )
```
